256 devices in a mesh: region: 128 (over z, y, x), level: 2 (over core).
Axes of the slice: x: 4, y: 4, z: 8, core: 2. Of those that a mesh axis runs over, the one named last changes fastest.
Arguments:
- latent: float32 [851968, 512], P('region', 'level'), may hold values from -6 to 6
- new_owner: int32 [6656], P('region'), may hold values from 0 to 127, as said below
- dest_slot: int32 [6656], P('region'), may hold values from 0 to 77, as said below
- live_rows: int32 [6656], P('region'), may hold values from 1 to 128
- norm_gain: float32 [512], P('level'), may hold values from 0.25 to 1.75
- w_in: bfloat16 [512, 512], replicated, may hold values from -0.25 to 0.25
- b_in: float32 [512], replicated, may hold values from -3 to 3
- w_out: bfloat16 [512, 512], P(None, 'level'), may hold values from -0.25 to 0.25
- b_out: float32 [512], P('level'), may hold values from -3 to 3
Outputs:
- updated: bfloat16 [1277952, 512], P('region', 'level')
The draws below stay inside these ranges and needn't reach their ends.
Inputs may be any that keep to these rules, and one draw needn't show every extreme that they name: `new_owner`: A region receives at most 78 blocks and one region hands at most 1 of its blocks to one region; both bounds are reached in every draw. `dest_slot`: blocks with the same new owner have different slots.
All inputs are finite; a program needn't handle non-finite values.
Results may differ from the reference program's by a relative error of at most 0.0045.
Values may be sent and summed in bfloat16 or wider, within the bound.
No kernel may reach another device: no remote copies, remote signals or barrier semaphores. Data moves between devices by JAX's collectives and lax.ppermute only.
A program may use at most 128 MiB of HBM per device.

```python
import jax
import jax.numpy as jnp
from jax import lax

D = 512
HID = 512
BLK = 128
OLD_DEV = 52
BLOCKS = 6656
NEW_CAP = 78
N_REGION = 128


def routing_plan(key):
    base = jax.random.fold_in(key, 7)
    excess_key, label_key, slot_key, order_key = jax.random.split(base, 4)
    regions = N_REGION
    pairs = regions // 2
    spare = NEW_CAP - OLD_DEV
    excess = jax.random.randint(excess_key, (pairs,), 0, spare + 1).astype(jnp.int32)
    excess = excess.at[0].set(spare)
    counts = jnp.concatenate([OLD_DEV + excess, OLD_DEV - excess])
    counts = counts[jax.random.permutation(label_key, regions)]
    ending = jnp.cumsum(counts).astype(jnp.int32)
    starting = ending - counts
    global_index = jnp.arange(regions * OLD_DEV, dtype=jnp.int32)
    receiver = jnp.sum((global_index[:, None] >= ending[None, :]).astype(jnp.int32), axis=1)
    position = global_index - starting[receiver]
    slot_table = jax.vmap(lambda subkey: jax.random.permutation(subkey, NEW_CAP))(jax.random.split(slot_key, regions)).astype(jnp.int32)
    slot_of = slot_table[receiver, position]
    sender = global_index % regions
    column = global_index // regions
    order_table = jax.vmap(lambda subkey: jax.random.permutation(subkey, OLD_DEV))(jax.random.split(order_key, regions)).astype(jnp.int32)
    block_index = sender * OLD_DEV + order_table[sender, column]
    owners = jnp.zeros((regions * OLD_DEV,), jnp.int32).at[block_index].set(receiver)
    slots = jnp.zeros((regions * OLD_DEV,), jnp.int32).at[block_index].set(slot_of)
    return (owners, slots)


def draw_new_owner(key, part):
    return routing_plan(key)[0]


def draw_dest_slot(key, part):
    return routing_plan(key)[1]


def touch_ends(entries, own_key, least, high):
    spot = [jax.random.randint(jax.random.fold_in(own_key, axis), (), 0, length) for axis, length in enumerate(entries.shape)]
    widest = entries.shape.index(max(entries.shape))
    beside = spot[:widest] + [(spot[widest] + 1) % entries.shape[widest]] + spot[widest + 1:]
    return entries.at[tuple(spot)].set(least).at[tuple(beside)].set(high)


def levels(stream_key, shape, cuts, least, largest):
    loudness, own = 1.0, jax.random.fold_in(stream_key, 6)
    for dim, parts in cuts:
        steps = jnp.exp(jax.random.uniform(jax.random.fold_in(own, dim), (parts,), jnp.float32, least / len(cuts), largest / len(cuts)))
        loudness = loudness * jnp.repeat(steps, shape[dim] // parts).reshape([-1 if axis == dim else 1 for axis in range(len(shape))])
    return loudness


def noise(stream_key, shape, deviation, bound, cuts=(), kind=jnp.bfloat16):
    level = levels(stream_key, shape, cuts, -0.22, 0.18) if cuts else 1.0
    values = jax.random.normal(stream_key, shape, jnp.float32) * deviation * level
    return jnp.minimum(jnp.maximum(values, -bound), bound).astype(kind)


def setup_inputs(seed: int = 0) -> dict:
    key_of = jax.random.split(jax.random.key(seed), 10)
    latent = noise(key_of[0], (BLOCKS * BLK, D), 1.0, 6.0, ((0, 128), (1, 2)), jnp.float32)
    new_owner = draw_new_owner(jax.random.fold_in(key_of[9], 71), 0)
    dest_slot = draw_dest_slot(jax.random.fold_in(key_of[9], 71), 0)
    live_rows = touch_ends(jax.random.randint(key_of[3], (BLOCKS,), 1, BLK + 1), jax.random.fold_in(key_of[3], 1), 1, BLK).astype(jnp.int32)
    norm_gain = jnp.clip(1.0 + 0.15 * jax.random.normal(key_of[4], (D,), jnp.float32), 0.25, 1.75)
    w_in = noise(key_of[5], (D, HID), D ** -0.5, 0.25)
    b_in = noise(key_of[6], (HID,), 0.5, 3.0, (), jnp.float32)
    w_out = noise(key_of[7], (HID, D), HID ** -0.5, 0.25, ((1, 2),))
    b_out = noise(key_of[8], (D,), 0.5, 3.0, ((0, 2),), jnp.float32)
    return {"latent": latent, "new_owner": new_owner, "dest_slot": dest_slot, "live_rows": live_rows, "norm_gain": norm_gain, "w_in": w_in, "b_in": b_in, "w_out": w_out, "b_out": b_out}


epsilon = 1e-05

def node_update(inputs, live, norm_gain, w_in, b_in, w_out, b_out):
    average = lax.optimization_barrier(jnp.sum(inputs, axis=1)) / D
    variance = lax.optimization_barrier(jnp.sum(inputs * inputs, axis=1)) / D - average * average
    normed = ((inputs - average[:, None]) * lax.rsqrt(variance + epsilon)[:, None] * norm_gain).astype(jnp.bfloat16)
    preact = jnp.dot(normed, w_in, preferred_element_type=jnp.float32) + b_in
    hidden = jax.nn.silu(preact).astype(jnp.bfloat16)
    result = jnp.dot(hidden, w_out, preferred_element_type=jnp.float32) + b_out + inputs
    keeping = (jnp.arange(BLK, dtype=jnp.int32)[None, :] < live[:, None]).reshape(-1)
    return jnp.where(keeping[:, None], result, 0.0).astype(jnp.bfloat16)

def reference(latent, new_owner, dest_slot, live_rows, norm_gain, w_in, b_in, w_out, b_out):
    grouped = latent.reshape(N_REGION, OLD_DEV * BLK, D)
    lives = live_rows.reshape(N_REGION, OLD_DEV)

    def per_region(pair):
        return node_update(pair[0], pair[1], norm_gain, w_in, b_in, w_out, b_out)
    done = lax.map(per_region, (grouped, lives)).reshape(N_REGION * OLD_DEV, BLK, D)
    target = (new_owner * NEW_CAP + dest_slot).astype(jnp.int32)
    updated = jnp.zeros((N_REGION * NEW_CAP, BLK, D), jnp.bfloat16).at[target].set(done)
    return updated.reshape(N_REGION * NEW_CAP * BLK, D)
```

```python
import functools

import jax
import jax.numpy as jnp
from jax import lax
from jax.experimental import pallas as pl
from jax.experimental.pallas import tpu as pltpu
from jax.sharding import PartitionSpec as P


epsilon = 1e-05
TILE = 16
PLANE = 16
CUTS = (0, 3, 6, 8)
FIRST = (27, 25, 15)
SECOND = (15, 15, 12)


def starts(sizes):
    out, at = [], 0
    for size in sizes:
        out.append(at)
        at += size
    return out


def mlp_kernel(level_ref, live_ref, mine_ref, theirs_ref, side_mine_ref, side_theirs_ref, w_in_ref,
               b_in_ref, w_mine_ref, w_theirs_ref, out_mine_ref, out_theirs_ref, *, block_rows, blocks, half_blocks):
    step = pl.program_id(0)
    level = level_ref[0]
    half = mine_ref.shape[1]
    mine, theirs = mine_ref[...], theirs_ref[...]
    width = 2 * half
    average = jnp.sum(mine + theirs, axis=1, keepdims=True) / width
    variance = jnp.sum(mine * mine + theirs * theirs, axis=1, keepdims=True) / width - average * average
    scale = lax.rsqrt(variance + epsilon)
    norm_mine = ((mine - average) * scale * side_mine_ref[0:1]).astype(jnp.bfloat16)
    norm_theirs = ((theirs - average) * scale * side_theirs_ref[0:1]).astype(jnp.bfloat16)
    at_mine = pl.multiple_of(level * half, half)
    at_theirs = pl.multiple_of((1 - level) * half, half)
    preact = (
        jnp.dot(norm_mine, w_in_ref[pl.ds(at_mine, half), :], preferred_element_type=jnp.float32)
        + jnp.dot(norm_theirs, w_in_ref[pl.ds(at_theirs, half), :], preferred_element_type=jnp.float32)
        + b_in_ref[...]
    )
    hidden = (preact / (1.0 + jnp.exp(-preact))).astype(jnp.bfloat16)
    row = lax.broadcasted_iota(jnp.int32, (block_rows, 1), 0)
    keeping = jnp.concatenate(
        [row < live_ref[level * half_blocks + step * blocks + i] for i in range(blocks)], axis=0
    )
    for w_ref, side_ref, rows, out_ref in (
        (w_mine_ref, side_mine_ref, mine, out_mine_ref),
        (w_theirs_ref, side_theirs_ref, theirs, out_theirs_ref),
    ):
        result = jnp.dot(hidden, w_ref[...], preferred_element_type=jnp.float32) + side_ref[1:2] + rows
        out_ref[...] = jnp.where(keeping, result, 0.0).astype(jnp.bfloat16)


def node_update(latent, live, norm_gain, w_in, b_in, w_out, b_out, old_blocks, block_rows):
    level = lax.axis_index("level")
    half_blocks = old_blocks // 2
    half_rows = half_blocks * block_rows
    width, half = latent.shape[1] * 2, latent.shape[1]
    hidden_width = w_in.shape[1]
    swap = [(0, 1), (1, 0)]
    sides = jnp.stack([norm_gain, b_out])
    going = lax.dynamic_slice_in_dim(latent, (1 - level) * half_rows, half_rows, 0)
    theirs = lax.ppermute(going, "level", swap)
    w_theirs = lax.ppermute(w_out, "level", swap)
    side_theirs = lax.ppermute(sides, "level", swap)
    blocks = 2
    rows = blocks * block_rows
    steps = half_rows // rows
    whole = lambda *shape: pl.BlockSpec(shape, lambda i, level_ref, live_ref: (0,) * len(shape))
    mlp = pl.pallas_call(
        functools.partial(mlp_kernel, block_rows=block_rows, blocks=blocks, half_blocks=half_blocks),
        grid_spec=pltpu.PrefetchScalarGridSpec(
            num_scalar_prefetch=2,
            grid=(steps,),
            in_specs=[
                pl.BlockSpec((rows, half), lambda i, level_ref, live_ref: (level_ref[0] * steps + i, 0)),
                pl.BlockSpec((rows, half), lambda i, level_ref, live_ref: (i, 0)),
                whole(2, half),
                whole(2, half),
                whole(width, hidden_width),
                whole(1, hidden_width),
                whole(hidden_width, half),
                whole(hidden_width, half),
            ],
            out_specs=[
                pl.BlockSpec((rows, half), lambda i, level_ref, live_ref: (i, 0)),
                pl.BlockSpec((rows, half), lambda i, level_ref, live_ref: (i, 0)),
            ],
        ),
        out_shape=[jax.ShapeDtypeStruct((half_rows, half), jnp.bfloat16)] * 2,
        name="node_mlp",
    )
    out_mine, out_theirs = mlp(level[None], live, latent, theirs, sides, side_theirs, w_in, b_in[None], w_out, w_theirs)
    return out_mine, lax.ppermute(out_theirs, "level", swap)


def plan_kernel(where_ref, table_ref, own_ref, fits_ref, pack_ref, relay_ref, place_ref, pos_ref, goal_ref):
    spot, depth = where_ref[0], where_ref[1]
    lanes = table_ref.shape[1]
    planes = lanes // PLANE
    tiles = 8
    total = sum(FIRST)
    f32, bf16 = jnp.float32, jnp.bfloat16
    table = table_ref[...]
    count = (table & 15).astype(f32)
    slot = (table >> 4).astype(f32)
    i0 = lax.broadcasted_iota(jnp.int32, (lanes, lanes), 0)
    i1 = lax.broadcasted_iota(jnp.int32, (lanes, lanes), 1)
    one = lambda mask: jnp.where(mask, 1.0, 0.0).astype(bf16)
    same = one(i0 // PLANE == i1 // PLANE)
    before = one((i0 // PLANE == i1 // PLANE) & (i0 < i1))
    above = one((i0 // planes == i1 // planes) & (i1 < i0))
    dot = lambda a, b: jnp.dot(a.astype(bf16), b.astype(bf16), preferred_element_type=f32)
    firsts, seconds = starts(FIRST), starts(SECOND)
    parts = range(len(FIRST))
    part_of = [c for c in parts for _ in range(CUTS[c], CUTS[c + 1])]
    fits = None
    run = []
    for c in parts:
        held = jnp.clip(count - CUTS[c], 0.0, float(CUTS[c + 1] - CUTS[c]))
        load = jnp.sum(held.reshape(lanes // planes, planes, lanes), axis=1)
        good = (jnp.max(dot(held, same)) <= FIRST[c]) & (jnp.max(load) <= SECOND[c])
        fits = good if fits is None else fits & good
        run.append(dot(above, held))
    fits_ref[0] = jnp.where(fits, 1, 0)
    lane = lax.broadcasted_iota(jnp.int32, (1, lanes), 1)
    within = (lane % PLANE).astype(f32)
    me = depth * PLANE + spot
    placed = jnp.zeros((lanes, lanes), f32)
    slot_col = jnp.sum(jnp.where(i1 == me, slot, 0.0), axis=1, keepdims=True)
    lane_f = i1.astype(f32)
    for t in range(tiles):
        c = part_of[t]
        here = count > t
        ahead = jnp.clip(count - CUTS[c], 0.0, float(t - CUTS[c]))
        pos = dot(ahead, same) + dot(jnp.where(here, 1.0, 0.0), before) + firsts[c]
        pos_ref[t] = jnp.where(here, pos, -1.0)
        order = run[c] + ahead
        goal_ref[t] = jnp.where(here, within * SECOND[c] + order + 1.0, 0.0)
        column = jnp.sum(jnp.where((i1 == me) & here, order + seconds[c] + 1.0, 0.0), axis=1, keepdims=True) - 1.0
        placed = placed + jnp.where(lane_f == column, slot_col * tiles + (t + 1.0), 0.0)
    place_ref[...] = jnp.sum(placed.reshape(lanes // planes, planes, lanes), axis=1).astype(jnp.int32) - 1
    down = lax.broadcasted_iota(jnp.int32, (total, lanes), 0).astype(f32)
    across = lax.broadcasted_iota(jnp.int32, (total, lanes), 1)
    own = own_ref[...].astype(f32)
    my_row = spot * planes + depth
    block_sum = jnp.zeros((total, lanes), f32)
    tile_sum = jnp.zeros((total, lanes), f32)
    for t in range(tiles):
        hit = pos_ref[t, pl.ds(my_row, 1), :] == down
        block_sum = block_sum + jnp.where(hit, own + 1.0, 0.0)
        tile_sum = tile_sum + jnp.where(hit, float(t), 0.0)
    gather = one(i0 // PLANE == i1)
    pack_ref[...] = ((dot(block_sum, gather) - 1.0) * tiles + dot(tile_sum, gather)).astype(jnp.int32)
    relay = jnp.zeros((total, lanes), f32)
    my_class = lane // PLANE == depth
    for z in range(planes):
        row = spot * planes + z
        got = jnp.zeros((total, lanes), f32)
        for t in range(tiles):
            hit = (pos_ref[t, pl.ds(row, 1), :] == down) & my_class
            got = got + jnp.where(hit, goal_ref[t, pl.ds(row, 1), :], 0.0)
        relay = jnp.where(across == z, jnp.sum(got, axis=1, keepdims=True), relay)
    relay_ref[...] = relay.astype(jnp.int32) - 1


def make_plan(where, table, own):
    lanes = table.shape[1]
    total = sum(FIRST)
    return pl.pallas_call(
        plan_kernel,
        in_specs=[pl.BlockSpec(memory_space=pltpu.SMEM), pl.BlockSpec(memory_space=pltpu.VMEM), pl.BlockSpec(memory_space=pltpu.VMEM)],
        out_specs=[pl.BlockSpec(memory_space=pltpu.SMEM)] + [pl.BlockSpec(memory_space=pltpu.VMEM)] * 3,
        out_shape=[
            jax.ShapeDtypeStruct((1,), jnp.int32),
            jax.ShapeDtypeStruct((total, lanes), jnp.int32),
            jax.ShapeDtypeStruct((total, lanes), jnp.int32),
            jax.ShapeDtypeStruct((PLANE, lanes), jnp.int32),
        ],
        scratch_shapes=[
            pltpu.VMEM((8, lanes, lanes), jnp.float32),
            pltpu.VMEM((8, lanes, lanes), jnp.float32),
        ],
        name="plan",
    )(where, table, own)


def finish(copy, started):
    lax.fori_loop(0, started, lambda _, carry: (copy.wait(), carry)[1], 0)


def pack_kernel(where_ref, pack_ref, mine_ref, theirs_ref, *rest, first, planes):
    outs, done = rest[:-1], rest[-1]
    depth, level = where_ref[1], where_ref[2]
    half_tiles = mine_ref.shape[0]
    size = outs[0].shape[0]
    started = jnp.int32(0)
    for k in range(planes):
        goal = lax.rem(depth + k, planes)

        def body(p, started, k=k, goal=goal):
            item = pack_ref[first + p, goal]
            near = item - level * half_tiles
            far = item - (1 - level) * half_tiles

            @pl.when((item >= 0) & (near >= 0) & (near < half_tiles))
            def _():
                pltpu.make_async_copy(mine_ref.at[near], outs[k].at[p], done).start()

            @pl.when((item >= 0) & (far >= 0) & (far < half_tiles))
            def _():
                pltpu.make_async_copy(theirs_ref.at[far], outs[k].at[p], done).start()

            return started + jnp.where(item >= 0, 1, 0)

        started = lax.fori_loop(0, size, body, started)
    finish(pltpu.make_async_copy(mine_ref.at[0], outs[0].at[0], done), started)


def relay_kernel(where_ref, relay_ref, *rest, first, planes):
    ins, out_ref, done = rest[:planes], rest[planes], rest[planes + 1]
    depth = where_ref[1]
    size = ins[0].shape[0]
    started = jnp.int32(0)
    for k in range(planes):
        source = lax.rem(depth + planes - k, planes)

        def body(p, started, k=k, source=source):
            item = relay_ref[first + p, source]

            @pl.when(item >= 0)
            def _():
                pltpu.make_async_copy(ins[k].at[p], out_ref.at[item], done).start()

            return started + jnp.where(item >= 0, 1, 0)

        started = lax.fori_loop(0, size, body, started)
    finish(pltpu.make_async_copy(ins[0].at[0], out_ref.at[0], done), started)


def place_kernel(place_ref, got_ref, _, out_ref, done, *, first, size):
    def outer(s, started):
        def body(q, started):
            item = place_ref[s, first + q]

            @pl.when(item >= 0)
            def _():
                pltpu.make_async_copy(got_ref.at[s * size + q], out_ref.at[item], done).start()

            return started + jnp.where(item >= 0, 1, 0)

        return lax.fori_loop(0, size, body, started)

    started = lax.fori_loop(0, PLANE, outer, jnp.int32(0))
    finish(pltpu.make_async_copy(got_ref.at[0], out_ref.at[0], done), started)


smem = pl.BlockSpec(memory_space=pltpu.SMEM)
anywhere = pl.BlockSpec(memory_space=pl.ANY)
vmem = pl.BlockSpec(memory_space=pltpu.VMEM)


def two_hops(where, pack, relay, place, mine, theirs, slot_count, block_rows, plane_groups, region_count):
    half = mine.shape[1]
    planes = region_count // PLANE
    tile = lambda n: jax.ShapeDtypeStruct((n, TILE, half), jnp.bfloat16)
    mine, theirs = mine.reshape(-1, TILE, half), theirs.reshape(-1, TILE, half)
    firsts, seconds = starts(FIRST), starts(SECOND)
    arrived = []
    for c, size in enumerate(FIRST):
        sent = pl.pallas_call(
            functools.partial(pack_kernel, first=firsts[c], planes=planes),
            in_specs=[smem, smem, vmem, vmem],
            out_specs=[anywhere] * planes,
            out_shape=[tile(size)] * planes,
            scratch_shapes=[pltpu.SemaphoreType.DMA(())],
            name="pack",
        )(where, pack, mine, theirs)
        where, _ = lax.optimization_barrier((where, sent[0]))
        came = [sent[0]]
        for k in range(1, planes):
            came.append(
                lax.ppermute(sent[k], "region", [(i, (i + k * PLANE) % region_count) for i in range(region_count)])
            )
        arrived.append(came)
    out = jnp.zeros((slot_count * block_rows // TILE, TILE, half), jnp.bfloat16)
    for c, size in enumerate(FIRST):
        onward = pl.pallas_call(
            functools.partial(relay_kernel, first=firsts[c], planes=planes),
            in_specs=[smem, smem] + [vmem] * planes,
            out_specs=anywhere,
            out_shape=tile(PLANE * SECOND[c]),
            scratch_shapes=[pltpu.SemaphoreType.DMA(())],
            name="relay",
        )(where, relay, *arrived[c])
        where, _ = lax.optimization_barrier((where, onward))
        got = lax.all_to_all(
            onward.reshape(PLANE, SECOND[c], TILE, half), "region", 0, 0, axis_index_groups=plane_groups, tiled=True
        ).reshape(-1, TILE, half)
        out = pl.pallas_call(
            functools.partial(place_kernel, first=seconds[c], size=SECOND[c]),
            in_specs=[smem, vmem, anywhere],
            out_specs=anywhere,
            out_shape=jax.ShapeDtypeStruct(out.shape, out.dtype),
            input_output_aliases={2: 0},
            scratch_shapes=[pltpu.SemaphoreType.DMA(())],
            name="place",
        )(place, got, out)
    return out.reshape(slot_count * block_rows, half)


def one_hop(table, new_owner, level, me, mine, theirs, slot_count, block_rows, old_blocks):
    region_count = table.shape[1]
    half = mine.shape[1]
    planes = region_count // PLANE
    first = jnp.where(level == 0, mine, theirs)
    last = jnp.where(level == 0, theirs, mine)
    finished = jnp.concatenate([first, last]).reshape(old_blocks, block_rows, half)
    send = jnp.zeros((region_count, block_rows, half), jnp.bfloat16).at[new_owner].set(finished)
    got = lax.all_to_all(send, "region", 0, 0, tiled=True)
    mine_col = lax.dynamic_index_in_dim(table, me, 1, keepdims=False)
    mine_col = mine_col.reshape(PLANE, planes).T.reshape(-1)
    slots = jnp.where(mine_col > 0, mine_col >> 4, slot_count)
    arrived = jnp.zeros((slot_count, block_rows, half), jnp.bfloat16).at[slots].set(got, mode="drop")
    return arrived.reshape(slot_count * block_rows, half)


def update_and_move(latent, new_owner, dest_slot, live_rows, norm_gain, w_in, b_in, w_out, b_out):
    region_count = lax.axis_size("region")
    planes = region_count // PLANE
    old_blocks = new_owner.shape[0]
    block_rows = latent.shape[0] // old_blocks
    slot_count = old_blocks + old_blocks // 2
    me = lax.axis_index("region")
    level = lax.axis_index("level")
    spot, depth = me % PLANE, me // PLANE
    where = jnp.stack([spot, depth, level]).astype(jnp.int32)
    depth_groups = [[z * PLANE + p for z in range(planes)] for p in range(PLANE)]
    plane_groups = [[z * PLANE + p for p in range(PLANE)] for z in range(planes)]

    tiles = (live_rows + (TILE - 1)) // TILE
    named = new_owner[:, None] == jnp.arange(region_count, dtype=jnp.int32)[None, :]
    entry = jnp.sum(jnp.where(named, (tiles + 16 * dest_slot)[:, None], 0), axis=0)
    own = jnp.sum(jnp.where(named, jnp.arange(old_blocks, dtype=jnp.int32)[:, None], 0), axis=0)
    spread = jnp.broadcast_to(entry[None], (planes, region_count))
    spread = lax.all_to_all(spread, "region", 0, 0, axis_index_groups=depth_groups, tiled=True)
    spread = jnp.broadcast_to(spread[None], (PLANE, planes, region_count))
    table = lax.all_to_all(spread, "region", 0, 0, axis_index_groups=plane_groups, tiled=True)
    table = table.reshape(region_count, region_count)
    fits, pack, relay, place = make_plan(where, table, own[None])

    mine, theirs = node_update(
        latent, live_rows, norm_gain, w_in, b_in, w_out, b_out, old_blocks, block_rows
    )
    return lax.cond(
        fits[0] > 0,
        lambda: two_hops(where, pack, relay, place, mine, theirs, slot_count, block_rows, plane_groups, region_count),
        lambda: one_hop(table, new_owner, level, me, mine, theirs, slot_count, block_rows, old_blocks),
    )


def solution(mesh):
    placed = (
        P("region", "level"),
        P("region"),
        P("region"),
        P("region"),
        P("level"),
        P(),
        P(),
        P(None, "level"),
        P("level"),
    )
    return jax.shard_map(update_and_move, mesh=mesh, in_specs=placed, out_specs=P("region", "level"), check_vma=False)
```
